8 devices in a mesh: rep: 1 (over z), pool: 8 (over y, x, core).
Axes of the slice: x: 2, y: 2, z: 1, core: 2. Of those that a mesh axis runs over, the one named last changes fastest.
Arguments:
- kv_pool: bfloat16 [4, 256, 2, 64, 20, 128], P(None, ('rep', 'pool'))
- page_idx: int32 [8, 8, 4], P(None, ('rep', 'pool'))
- tok_hidden: bfloat16 [8, 128, 2560], P(('rep', 'pool'))
- attn_norm: bfloat16 [4, 2560], replicated
- w_query: bfloat16 [4, 2560, 2560], replicated
- w_key: bfloat16 [4, 2560, 2560], replicated
- w_value: bfloat16 [4, 2560, 2560], replicated
- w_out: bfloat16 [4, 2560, 2560], replicated
- mlp_norm: bfloat16 [4, 2560], replicated
- w_gate: bfloat16 [4, 2560, 6912], replicated
- w_up: bfloat16 [4, 2560, 6912], replicated
- w_down: bfloat16 [4, 6912, 2560], replicated
Outputs:
- output: bfloat16 [8, 128, 2560], P(('rep', 'pool'))
All inputs are finite; a program needn't handle non-finite values.
Results may differ from the reference program's by a relative error of at most 0.02.
Values are sent between devices in bfloat16 or wider.
A program may use at most 2.75 GiB of HBM per device.

```python
import math
import jax
import jax.numpy as jnp
from jax import lax

GROUP = 8
LAYERS = 4
TOKENS = 128
PAGE_LEN = 64
SLOTS = 4
POOL_PAGES = 32
HIDDEN = 2560
NUM_HEADS = 20
HEAD_DIM = 128
FF_DIM = 6912
ROPE_BASE = 10000

PREFIX = GROUP * SLOTS * PAGE_LEN
ATTN_WIDTH = NUM_HEADS * HEAD_DIM


def setup_inputs(seed: int = 0, part: int = 0) -> dict:
    part_key = jax.random.fold_in(jax.random.key(seed), part)
    pool_key, idx_key, hid_key = jax.random.split(part_key, 3)
    weight_keys = jax.random.split(jax.random.key(seed + 1), 9)
    kv_pool = jax.random.normal(pool_key, (LAYERS, GROUP * POOL_PAGES, 2, PAGE_LEN, NUM_HEADS, HEAD_DIM), jnp.float32).astype(jnp.bfloat16)
    owner_keys = jax.random.split(idx_key, GROUP)
    page_perm = jax.vmap(lambda owner_key: jax.random.permutation(owner_key, POOL_PAGES))(owner_keys)
    chosen = page_perm[:, : GROUP * SLOTS].reshape(GROUP, GROUP, SLOTS)
    page_idx = jnp.transpose(chosen, (1, 0, 2)).astype(jnp.int32)
    tok_hidden = jax.random.normal(hid_key, (GROUP, TOKENS, HIDDEN), jnp.float32).astype(jnp.bfloat16)

    def make_weight(key, shape, fan_in, gain):
        return (jax.random.normal(key, shape, jnp.float32) * (gain / math.sqrt(fan_in))).astype(jnp.bfloat16)

    def make_gain(key):
        return (1.0 + 0.3 * jax.random.normal(key, (LAYERS, HIDDEN), jnp.float32)).astype(jnp.bfloat16)

    return {
        'kv_pool': kv_pool,
        'page_idx': page_idx,
        'tok_hidden': tok_hidden,
        'attn_norm': make_gain(weight_keys[0]),
        'w_query': make_weight(weight_keys[1], (LAYERS, HIDDEN, ATTN_WIDTH), HIDDEN, 2.5),
        'w_key': make_weight(weight_keys[2], (LAYERS, HIDDEN, ATTN_WIDTH), HIDDEN, 1.0),
        'w_value': make_weight(weight_keys[3], (LAYERS, HIDDEN, ATTN_WIDTH), HIDDEN, 1.0),
        'w_out': make_weight(weight_keys[4], (LAYERS, ATTN_WIDTH, HIDDEN), ATTN_WIDTH, 1.0),
        'mlp_norm': make_gain(weight_keys[5]),
        'w_gate': make_weight(weight_keys[6], (LAYERS, HIDDEN, FF_DIM), HIDDEN, 1.0),
        'w_up': make_weight(weight_keys[7], (LAYERS, HIDDEN, FF_DIM), HIDDEN, 1.0),
        'w_down': make_weight(weight_keys[8], (LAYERS, FF_DIM, HIDDEN), FF_DIM, 1.0),
    }


def rms_norm(vals, gain):
    vals_f = vals.astype(jnp.float32)
    inv_rms = lax.rsqrt(jnp.mean(vals_f * vals_f, axis=-1, keepdims=True) + 1e-6)
    return (vals_f * inv_rms * gain.astype(jnp.float32)).astype(jnp.bfloat16)


def rope_tables():
    positions = (PREFIX + jnp.arange(TOKENS)).astype(jnp.float32)
    exponent = jnp.arange(HEAD_DIM // 2).astype(jnp.float32) * (-2.0 / HEAD_DIM)
    inv_freq = jnp.power(float(ROPE_BASE), exponent)
    angles = positions[:, None] * inv_freq[None, :]
    return jnp.cos(angles)[:, None, :], jnp.sin(angles)[:, None, :]


def apply_rope(proj, cosine, sine):
    half = HEAD_DIM // 2
    first = proj[..., :half]
    second = proj[..., half:]
    return jnp.concatenate([first * cosine - second * sine, second * cosine + first * sine], axis=-1)


def reference(kv_pool, page_idx, tok_hidden, attn_norm, w_query, w_key, w_value, w_out, mlp_norm, w_gate, w_up, w_down):
    cosine, sine = rope_tables()
    owner_base = (jnp.arange(GROUP) * POOL_PAGES)[:, None]
    causal = jnp.arange(TOKENS)[None, :] <= jnp.arange(TOKENS)[:, None]
    visible = jnp.concatenate([jnp.full((TOKENS, PREFIX), True), causal], axis=1)
    scale = 1.0 / math.sqrt(HEAD_DIM)
    layer_stack = (kv_pool, attn_norm, w_query, w_key, w_value, w_out, mlp_norm, w_gate, w_up, w_down)
    head_shape = (TOKENS, NUM_HEADS, HEAD_DIM)

    def one_request(request_in):
        tok_rows, page_rows = request_in
        flat_pages = (page_rows + owner_base).reshape(GROUP * SLOTS)

        def layer_step(hidden, layer_in):
            layer_pool, gain_attn, q_weight, k_weight, v_weight, o_weight, gain_mlp, gate_weight, up_weight, down_weight = layer_in
            fetched = layer_pool[flat_pages]
            key_pre = fetched[:, 0].reshape(PREFIX, NUM_HEADS, HEAD_DIM)
            val_pre = fetched[:, 1].reshape(PREFIX, NUM_HEADS, HEAD_DIM)
            normed = rms_norm(hidden, gain_attn)
            query = apply_rope(jnp.dot(normed, q_weight, preferred_element_type=jnp.float32).reshape(head_shape), cosine, sine).astype(jnp.bfloat16)
            key_new = apply_rope(jnp.dot(normed, k_weight, preferred_element_type=jnp.float32).reshape(head_shape), cosine, sine).astype(jnp.bfloat16)
            val_new = jnp.dot(normed, v_weight, preferred_element_type=jnp.float32).astype(jnp.bfloat16).reshape(head_shape)
            keys_all = jnp.concatenate([key_pre, key_new], axis=0)
            vals_all = jnp.concatenate([val_pre, val_new], axis=0)
            scores = jnp.einsum('thd,nhd->htn', query.astype(jnp.float32), keys_all.astype(jnp.float32)) * scale
            scores = jnp.where(visible[None, :, :], scores, -1e30)
            attn_prob = jax.nn.softmax(scores, axis=-1).astype(jnp.bfloat16)
            mixed = jnp.einsum('htn,nhd->thd', attn_prob.astype(jnp.float32), vals_all.astype(jnp.float32))
            attn_out = mixed.astype(jnp.bfloat16).reshape(TOKENS, ATTN_WIDTH)
            hidden = (hidden.astype(jnp.float32) + jnp.dot(attn_out, o_weight, preferred_element_type=jnp.float32)).astype(jnp.bfloat16)
            normed_mlp = rms_norm(hidden, gain_mlp)
            gate = jnp.dot(normed_mlp, gate_weight, preferred_element_type=jnp.float32)
            upper = jnp.dot(normed_mlp, up_weight, preferred_element_type=jnp.float32)
            inner = (jax.nn.silu(gate) * upper).astype(jnp.bfloat16)
            hidden = (hidden.astype(jnp.float32) + jnp.dot(inner, down_weight, preferred_element_type=jnp.float32)).astype(jnp.bfloat16)
            return hidden, None

        out_rows, _ = lax.scan(layer_step, tok_rows, layer_stack)
        return out_rows

    return lax.map(one_request, (tok_hidden, page_idx))
```

```python
import functools
import math
import jax
import jax.numpy as jnp
from jax import lax
from jax.experimental import pallas as pl
from jax.experimental.pallas import tpu as pltpu
from jax.sharding import PartitionSpec as P

NORM_EPS = 1e-6
ROPE_BASE = 10000.0
GROUP_HEADS = 2
Q_AHEAD = 3
MESH = pl.DeviceIdType.MESH


def rope_tables(offset, tokens, head_dim):
    positions = (offset + jnp.arange(tokens)).astype(jnp.float32)
    exponent = jnp.arange(head_dim // 2).astype(jnp.float32) * (-2.0 / head_dim)
    inv_freq = jnp.power(ROPE_BASE, exponent)
    angles = positions[:, None] * inv_freq[None, :]
    cosine, sine = jnp.cos(angles), jnp.sin(angles)
    return jnp.concatenate([cosine, cosine], axis=-1), jnp.concatenate([-sine, sine], axis=-1)


def rms_rows(vals, gain):
    inv_rms = lax.rsqrt(jnp.mean(vals * vals, axis=-1, keepdims=True) + NORM_EPS)
    return (vals * inv_rms * gain).astype(jnp.bfloat16)


def qkv_kernel(layer, head_dim, x_ref, gain_ref, cos_ref, sin_ref, wq_ref, wk_ref, wv_ref, q_ref, k_ref, v_ref, h_ref):
    @pl.when(pl.program_id(0) == 0)
    def _():
        h_ref[...] = rms_rows(x_ref[...].astype(jnp.float32), gain_ref[layer : layer + 1, :].astype(jnp.float32))

    normed = h_ref[...]
    cosine, sine = cos_ref[...], sin_ref[...]
    for w_ref, o_ref in ((wq_ref, q_ref), (wk_ref, k_ref)):
        proj = jnp.dot(normed, w_ref[...], preferred_element_type=jnp.float32)
        for h in range(GROUP_HEADS):
            part = proj[:, h * head_dim : (h + 1) * head_dim]
            turned = part * cosine + pltpu.roll(part, head_dim // 2, 1) * sine
            o_ref[:, h * head_dim : (h + 1) * head_dim] = turned.astype(jnp.bfloat16)
    v_ref[...] = jnp.dot(normed, wv_ref[...], preferred_element_type=jnp.float32).astype(jnp.bfloat16)


def project_qkv(layer, hidden, gain, cosine, sine, wq, wk, wv, head_dim):
    tokens, width = hidden.shape
    cols = GROUP_HEADS * head_dim
    steps = wq.shape[2] // cols
    whole = lambda a: pl.BlockSpec(a.shape, lambda j: (0,) * a.ndim)
    wspec = pl.BlockSpec((None, width, cols), lambda j: (layer, 0, j))
    ospec = pl.BlockSpec((None, tokens, cols), lambda j: (j, 0, 0))
    oshape = jax.ShapeDtypeStruct((steps, tokens, cols), jnp.bfloat16)
    return pl.pallas_call(
        functools.partial(qkv_kernel, layer, head_dim),
        grid=(steps,),
        in_specs=[whole(hidden), whole(gain), whole(cosine), whole(sine), wspec, wspec, wspec],
        out_specs=[ospec] * 3,
        out_shape=[oshape] * 3,
        scratch_shapes=[pltpu.VMEM((tokens, width), jnp.bfloat16)],
        compiler_params=pltpu.CompilerParams(dimension_semantics=("arbitrary",)),
        name="qkv",
    )(hidden, gain, cosine, sine, wq, wk, wv)


def mlp_kernel(layer, o_steps, o_cols, x_ref, a_ref, gain_ref, wo_ref, wg_ref, wu_ref, wd_ref, out_ref, x1_ref, h_ref, acc_ref):
    step = pl.program_id(0)

    @pl.when(step < o_steps)
    def _():
        cols = pl.ds(pl.multiple_of(step * o_cols, o_cols), o_cols)
        proj = jnp.dot(a_ref[...], wo_ref[...], preferred_element_type=jnp.float32)
        x1_ref[:, cols] = (x_ref[:, cols].astype(jnp.float32) + proj).astype(jnp.bfloat16)

    @pl.when(step == o_steps)
    def _():
        h_ref[...] = rms_rows(x1_ref[...].astype(jnp.float32), gain_ref[layer : layer + 1, :].astype(jnp.float32))
        acc_ref[...] = jnp.zeros_like(acc_ref)

    @pl.when(step >= o_steps)
    def _():
        normed = h_ref[...]
        gate = jnp.dot(normed, wg_ref[...], preferred_element_type=jnp.float32)
        upper = jnp.dot(normed, wu_ref[...], preferred_element_type=jnp.float32)
        inner = (jax.nn.silu(gate) * upper).astype(jnp.bfloat16)
        acc_ref[...] += jnp.dot(inner, wd_ref[...], preferred_element_type=jnp.float32)

    @pl.when(step == pl.num_programs(0) - 1)
    def _():
        out_ref[...] = (x1_ref[...].astype(jnp.float32) + acc_ref[...]).astype(jnp.bfloat16)


def out_and_mlp(layer, hidden, attn, gain, wo, wg, wu, wd):
    tokens, width = hidden.shape
    o_cols, f_cols = 256, 384
    o_steps, f_steps = width // o_cols, wg.shape[2] // f_cols
    whole = lambda a: pl.BlockSpec(a.shape, lambda j: (0,) * a.ndim)
    ff = lambda j: jnp.maximum(j - o_steps, 0)
    return pl.pallas_call(
        functools.partial(mlp_kernel, layer, o_steps, o_cols),
        grid=(o_steps + f_steps,),
        in_specs=[
            whole(hidden),
            whole(attn),
            whole(gain),
            pl.BlockSpec((None, wo.shape[1], o_cols), lambda j: (layer, 0, jnp.minimum(j, o_steps - 1))),
            pl.BlockSpec((None, width, f_cols), lambda j: (layer, 0, ff(j))),
            pl.BlockSpec((None, width, f_cols), lambda j: (layer, 0, ff(j))),
            pl.BlockSpec((None, f_cols, width), lambda j: (layer, ff(j), 0)),
        ],
        out_specs=whole(hidden),
        out_shape=jax.ShapeDtypeStruct(hidden.shape, jnp.bfloat16),
        scratch_shapes=[
            pltpu.VMEM((tokens, width), jnp.bfloat16),
            pltpu.VMEM((tokens, width), jnp.bfloat16),
            pltpu.VMEM((tokens, width), jnp.float32),
        ],
        compiler_params=pltpu.CompilerParams(dimension_semantics=("arbitrary",)),
        name="out_mlp",
    )(hidden, attn, gain, wo, wg, wu, wd)


def stat_rows(maxes, sums):
    rows = [r for pair in zip(maxes, sums) for r in pair]
    index = lax.broadcasted_iota(jnp.int32, (8, rows[0].shape[-1]), 0)
    block = jnp.zeros((8, rows[0].shape[-1]), jnp.float32)
    for n, row in enumerate(rows):
        block = jnp.where(index == n, row, block)
    return block


def merge_into(dst, src, dim):
    base = GROUP_HEADS * dim
    one, two = dst[base : base + 8, :], src[base : base + 8, :]
    maxes, sums = [], []
    for h in range(GROUP_HEADS):
        m1, m2 = one[2 * h : 2 * h + 1], two[2 * h : 2 * h + 1]
        top = jnp.maximum(m1, m2)
        a1, a2 = jnp.exp2(m1 - top), jnp.exp2(m2 - top)
        rows = slice(h * dim, (h + 1) * dim)
        dst[rows, :] = dst[rows, :] * a1 + src[rows, :] * a2
        maxes.append(top)
        sums.append(one[2 * h + 1 : 2 * h + 2] * a1 + two[2 * h + 1 : 2 * h + 2] * a2)
    dst[base : base + 8, :] = stat_rows(maxes, sums)


def partial_attention(dst, query, key_of, val_of, scale, dim, mask=None):
    maxes, sums = [], []
    for h in range(GROUP_HEADS):
        score = lax.dot_general(
            key_of(h), query[:, h * dim : (h + 1) * dim], (((1,), (1,)), ((), ())), preferred_element_type=jnp.float32
        )
        score = score * scale
        if mask is not None:
            score = jnp.where(mask, score, -1e30)
        top = jnp.max(score, axis=0, keepdims=True)
        expo = jnp.exp2(score - top)
        sums.append(jnp.sum(expo, axis=0, keepdims=True))
        maxes.append(top)
        dst[h * dim : (h + 1) * dim, :] = lax.dot_general(
            val_of(h), expo.astype(jnp.bfloat16), (((0,), (0,)), ((), ())), preferred_element_type=jnp.float32
        )
    dst[GROUP_HEADS * dim : GROUP_HEADS * dim + 8, :] = stat_rows(maxes, sums)


def attn_kernel(
    layer, groups, dim,
    idx_ref, q_ref, kn_ref, vn_ref, kv_ref, a_ref,
    kvb, kvo, qall, part, prx, rel, fin,
    kv_sem, qs_sem, qr_sem, ps_sem, pr_sem, ds_sem, dr_sem, fs_sem, fr_sem,
):
    me = lax.axis_index("pool")
    rep = lax.axis_index("rep")
    core = me % 2
    xpos = (me // 2) % 2
    ypos = me // 4
    scale = math.log2(math.e) / math.sqrt(dim)
    tokens = q_ref.shape[1]
    page_len = kvb.shape[3]

    def at(flip_y, flip_x, flip_core):
        return (((ypos + flip_y) % 2) * 2 + (xpos + flip_x) % 2) * 2 + (core + flip_core) % 2

    mate, xdev, ydev = (rep, at(0, 0, 1)), (rep, at(0, 1, 0)), (rep, at(1, 0, 0))

    def remote(src, dst, ssem, rsem, dev):
        return pltpu.make_async_remote_copy(src, dst, ssem, rsem, device_id=dev, device_id_type=MESH)

    def q_own(n, g):
        slot, dev = ((1, xdev), (2, ydev), (4, mate))[n]
        return remote(q_ref.at[g], qall.at[slot, g], qs_sem.at[n, g], qr_sem.at[slot, g], dev)

    def q_mate(slot, g):
        return remote(qall.at[slot, g], qall.at[slot + 4, g], qs_sem.at[2 + slot, g], qr_sem.at[slot + 4, g], mate)

    def q_relay(via_x, g):
        slot, dev = (1, ydev) if via_x else (2, xdev)
        return remote(qall.at[slot, g], qall.at[3, g], qs_sem.at[6, g], qr_sem.at[3, g], dev)

    def to_mate(n, g):
        return remote(part.at[4 + n, g], prx.at[n, g], ps_sem.at[n, g], pr_sem.at[n, g], mate)

    def diag_send(via_x, g):
        return remote(part.at[3, g], rel.at[g], ds_sem.at[g], dr_sem.at[g], xdev if via_x else ydev)

    def home_send(n, g):
        return remote(part.at[1 + n, g], fin.at[n, g], fs_sem.at[n, g], fr_sem.at[n, g], xdev if n == 0 else ydev)

    def kv_copy(g):
        src = kv_ref.at[layer, :, :, pl.ds(g * GROUP_HEADS, GROUP_HEADS)]
        return pltpu.make_async_copy(src, kvb, kv_sem)

    kv_copy(0).start()

    barrier = pltpu.get_barrier_semaphore()
    for dev in (mate, xdev, ydev):
        pl.semaphore_signal(barrier, inc=1, device_id=dev, device_id_type=MESH)
    pl.semaphore_wait(barrier, 3)

    def send_own(g):
        for n in range(3):
            q_own(n, g).start()

    for g in range(Q_AHEAD):
        send_own(g)
    for g in range(groups):
        qall[0, g] = q_ref[g]

    def attend(g):
        kv_copy(g).wait()

        def order(rank, carry):
            request = at((rank // 2) % 2, rank % 2, rank // 4)
            for j in range(idx_ref.shape[1]):
                page = idx_ref[request, j]
                for side in range(2):
                    for h in range(GROUP_HEADS):
                        kvo[rank, side, h, j * page_len : (j + 1) * page_len, :] = kvb[page, side, h]
            return carry

        lax.fori_loop(0, 8, order, 0)

        @pl.when(g + 1 < groups)
        def _():
            kv_copy(g + 1).start()

        for s in range(4, 8):
            remote(qall.at[s, g], qall.at[s, g], qs_sem.at[0, g], qr_sem.at[s, g], mate).wait_recv()

        def half(turn, carry):
            other = 1 - turn
            for z in range(4):
                rank = other * 4 + z
                partial_attention(
                    part.at[rank, g], qall[rank, g], lambda h: kvo[rank, 0, h], lambda h: kvo[rank, 1, h], scale, dim
                )

            @pl.when(other == 1)
            def _():
                for n in range(4):
                    to_mate(n, g).start()

            return carry

        lax.fori_loop(0, 2, half, 0)
        cols = lambda h: slice(h * dim, (h + 1) * dim)
        key_row = lax.broadcasted_iota(jnp.int32, (tokens, tokens), 0)
        query_col = lax.broadcasted_iota(jnp.int32, (tokens, tokens), 1)
        partial_attention(
            part.at[8, g], q_ref[g], lambda h: kn_ref[g, :, cols(h)], lambda h: vn_ref[g, :, cols(h)],
            scale, dim, key_row <= query_col,
        )

    def finish(g):
        for n in range(2):
            home_send(n, g).wait_recv()
        blocks = [part.at[0, g], part.at[8, g], fin.at[0, g], fin.at[1, g]]
        base = GROUP_HEADS * dim
        stats = [b[base : base + 8, :] for b in blocks]
        for h in range(GROUP_HEADS):
            tops = [s[2 * h : 2 * h + 1] for s in stats]
            top = functools.reduce(jnp.maximum, tops)
            weights = [jnp.exp2(t - top) for t in tops]
            total = sum(w * s[2 * h + 1 : 2 * h + 2] for w, s in zip(weights, stats))
            mixed = sum(w * b[h * dim : (h + 1) * dim, :] for w, b in zip(weights, blocks)) / total
            cols = pl.ds(pl.multiple_of(g * base + h * dim, dim), dim)
            a_ref[:, cols] = jnp.transpose(mixed).astype(jnp.bfloat16)

    def stage(i, lag, fn):
        g = i - lag

        @pl.when(jnp.logical_and(g >= 0, g < groups))
        def _():
            fn(g)

    def both(g, fn):
        @pl.when(g % 2 == 0)
        def _():
            fn(True)

        @pl.when(g % 2 == 1)
        def _():
            fn(False)

    def relay_step(g):
        def run(via_x):
            diag_send(via_x, g).wait_recv()
            n = 1 if via_x else 0
            merge_into(part.at[1 + n, g], rel.at[g], dim)
            home_send(n, g).start()

        both(g, run)

    def merge_step(g):
        for n in (3, 1, 2, 0):
            to_mate(n, g).wait_recv()

        def run(via_x):
            merge_into(part.at[3, g], prx.at[3, g], dim)
            diag_send(via_x, g).start()
            first = 0 if via_x else 1
            merge_into(part.at[1 + first, g], prx.at[1 + first, g], dim)
            home_send(first, g).start()
            merge_into(part.at[2 - first, g], prx.at[2 - first, g], dim)

        both(g, run)
        merge_into(part.at[0, g], prx.at[0, g], dim)

    def q_first(g):
        @pl.when(g + Q_AHEAD < groups)
        def _():
            send_own(g + Q_AHEAD)

        for n in range(2):
            q_own(n, g).wait_recv()

        def run(via_x):
            q_relay(via_x, g).start()

        both(g, run)
        q_mate(1, g).start()
        q_mate(2, g).start()

    def q_second(g):
        q_relay(True, g).wait_recv()
        q_mate(3, g).start()

    def body(i, carry):
        stage(i, 4, relay_step)
        stage(i, 3, merge_step)
        stage(i, 0, q_first)
        stage(i, 1, q_second)
        stage(i, 2, attend)
        stage(i, 5, finish)
        return carry

    lax.fori_loop(0, groups + 5, body, 0)

    def drain(g, carry):
        for n in range(3):
            q_own(n, g).wait_send()
            q_mate(1 + n, g).wait_send()
        q_relay(True, g).wait_send()
        for n in range(4):
            to_mate(n, g).wait_send()
        diag_send(True, g).wait_send()
        for n in range(2):
            home_send(n, g).wait_send()
        return carry

    lax.fori_loop(0, groups, drain, 0)


def attention(layer, idx, query, key_new, val_new, kv):
    groups, tokens, cols = query.shape
    dim = cols // GROUP_HEADS
    pages, page_len = kv.shape[1], kv.shape[4]
    rows = cols + 8
    dma = pltpu.SemaphoreType.DMA
    vmem = pl.BlockSpec(memory_space=pltpu.VMEM)
    return pl.pallas_call(
        functools.partial(attn_kernel, layer, groups, dim),
        in_specs=[pl.BlockSpec(memory_space=pltpu.SMEM), vmem, vmem, vmem, pl.BlockSpec(memory_space=pl.ANY)],
        out_specs=vmem,
        out_shape=jax.ShapeDtypeStruct((tokens, groups * cols), jnp.bfloat16),
        scratch_shapes=[
            pltpu.VMEM((pages, 2, GROUP_HEADS, page_len, dim), jnp.bfloat16),
            pltpu.VMEM((8, 2, GROUP_HEADS, idx.shape[1] * page_len, dim), jnp.bfloat16),
            pltpu.VMEM((8, groups, tokens, cols), jnp.bfloat16),
            pltpu.VMEM((9, groups, rows, tokens), jnp.float32),
            pltpu.VMEM((4, groups, rows, tokens), jnp.float32),
            pltpu.VMEM((groups, rows, tokens), jnp.float32),
            pltpu.VMEM((2, groups, rows, tokens), jnp.float32),
            dma,
            dma((7, groups)),
            dma((8, groups)),
            dma((4, groups)),
            dma((4, groups)),
            dma((groups,)),
            dma((groups,)),
            dma((2, groups)),
            dma((2, groups)),
        ],
        compiler_params=pltpu.CompilerParams(collective_id=layer, has_side_effects=True, vmem_limit_bytes=60 << 20),
        name="attn",
    )(idx, query, key_new, val_new, kv)


def solution(mesh):
    group = mesh.shape["pool"]

    def local_program(kv_local, idx_local, hid_local, attn_norm, w_query, w_key, w_value, w_out, mlp_norm, w_gate, w_up, w_down):
        head_dim = kv_local.shape[-1]
        prefix = group * idx_local.shape[2] * kv_local.shape[3]
        cosine, sine = rope_tables(prefix, hid_local.shape[1], head_dim)
        kv = jnp.transpose(kv_local, (0, 1, 2, 4, 3, 5))
        idx = idx_local[:, 0, :]
        hidden = hid_local[0]
        for layer in range(kv_local.shape[0]):
            query, key_new, val_new = project_qkv(layer, hidden, attn_norm, cosine, sine, w_query, w_key, w_value, head_dim)
            attn = attention(layer, idx, query, key_new, val_new, kv)
            hidden = out_and_mlp(layer, hidden, attn, mlp_norm, w_out, w_gate, w_up, w_down)
        return hidden[None]

    data_specs = (P(None, ("rep", "pool")), P(None, ("rep", "pool"), None), P(("rep", "pool")))
    return jax.shard_map(local_program, mesh=mesh, in_specs=data_specs + (P(),) * 9, out_specs=P(("rep", "pool")), check_vma=False)
```
